256 devices in a mesh: section: 4 (over z_lo), dp: 32 (over x, y, core), tensor: 2 (over z_hi).
Axes of the slice: x: 4, y: 4, z: 8 (z_hi: 2, z_lo: 4; z = z_hi * 4 + z_lo), core: 2. Of those that a mesh axis runs over, the one named last changes fastest.
Arguments:
- inputs: bfloat16 [2, 4096, 768], P(None, 'dp'), may hold values from -6 to 6
- out_grads: bfloat16 [2, 4096, 768], P(None, 'dp'), may hold values from -6 to 6
- norm_gain: float32 [4, 768], P('section'), may hold values from 0.1 to 1.9
- up_weight: bfloat16 [4, 768, 3072], P('section', None, 'tensor'), may hold values from -0.21875 to 0.21875
- down_weight: bfloat16 [4, 3072, 768], P('section', 'tensor'), may hold values from -0.109375 to 0.109375
- prior_up_grad: bfloat16 [32, 4, 768, 3072], P('dp', 'section', None, 'tensor'), may hold values from -6 to 6
- prior_down_grad: bfloat16 [32, 4, 3072, 768], P('dp', 'section', 'tensor'), may hold values from -6 to 6
- master_up: float32 [4, 768, 3072], P('section', 'dp', 'tensor'), may hold values from -0.3 to 0.3
- master_down: float32 [4, 3072, 768], P('section', ('tensor', 'dp')), may hold values from -0.3 to 0.3
Outputs:
- layer_outputs: bfloat16 [4, 2, 4096, 768], P('section', None, 'dp')
- input_grads: bfloat16 [4, 2, 4096, 768], P('section', None, 'dp')
- new_up: float32 [4, 768, 3072], P('section', 'dp', 'tensor')
- new_down: float32 [4, 3072, 768], P('section', ('tensor', 'dp'))
The draws below stay inside these ranges and needn't reach their ends.
All inputs are finite; a program needn't handle non-finite values.
Results may differ from the reference program's by a relative error of at most 0.019.
Values may be sent and summed in bfloat16 or wider, within the bound.
No kernel may reach another device: no remote copies, remote signals or barrier semaphores. Data moves between devices by JAX's collectives and lax.ppermute only.
A program may use at most 128 MiB of HBM per device.

```python
import jax
import jax.numpy as jnp
from jax import lax

D = 768
FF = 3072
MICRO = 2
LAYERS = 4
TOKENS = 4096
N_DP = 32


def strengthened(result, stream_key, source, target, parts, factor):
    def block_of(position):
        return (jnp.arange(result.shape[position]) // (result.shape[position] // parts)).reshape((-1,) + (1,) * (result.ndim - 1 - position))

    one_side = jax.random.permutation(stream_key, parts)[block_of(target)]
    other_side = (block_of(target) + parts // 2) % parts
    return jnp.where((block_of(source) == one_side) | (block_of(source) == other_side), factor * result, result)


def block_scale(rng, shape, shards, low, top_value):
    def one(position, shards_of):
        draws = jax.random.uniform(jax.random.fold_in(jax.random.fold_in(rng, 6), position), (shards_of,), jnp.float32, low / len(shards), top_value / len(shards))
        return jnp.repeat(jnp.exp(draws), shape[position] // shards_of).reshape((-1,) + (1,) * (len(shape) - position - 1))

    factor_of = one(*shards[0])
    for cut in shards[1:]:
        factor_of = factor_of * one(*cut)
    return factor_of


def centred(stream_key, dims, scale, most, pieces=(), dtype=jnp.bfloat16):
    loudness = block_scale(stream_key, dims, pieces, -0.22, 0.18) if pieces else 1.0
    drawn = jax.random.normal(stream_key, dims, jnp.float32) * scale * loudness
    return jnp.minimum(jnp.maximum(drawn, -most), most).astype(dtype)


def heavy_noise(rng, dims, scale, most, split, heavy, held_as=jnp.bfloat16):
    drawn = scale * jax.random.normal(rng, dims, jnp.float32)
    if split:
        drawn = drawn * block_scale(rng, dims, split, -0.22, 0.18)
    return jnp.clip(strengthened(drawn, jax.random.fold_in(rng, 3), *heavy), -most, most).astype(held_as)


def setup_inputs(seed: int = 0) -> dict:
    key_list = jax.random.split(jax.random.key(seed), 10)
    return {
        "inputs": centred(key_list[0], (MICRO, TOKENS, D), 1.0, 6.0, ((1, 32),)),
        "out_grads": centred(key_list[1], (MICRO, TOKENS, D), 1.0, 6.0, ((1, 32),)),
        "norm_gain": jnp.clip(1.0 + 0.18 * jax.random.normal(key_list[2], (LAYERS, D), jnp.float32), 0.1, 1.9),
        "up_weight": centred(key_list[3], (LAYERS, D, FF), D ** -0.5, 0.21875, ((0, 4), (2, 2))),
        "down_weight": centred(key_list[4], (LAYERS, FF, D), FF ** -0.5, 0.109375, ((0, 4), (1, 2))),
        "prior_up_grad": heavy_noise(key_list[5], (N_DP, LAYERS, D, FF), 1.0, 6.0, ((0, 32), (1, 4), (3, 2)), (0, 2, 32, 2.75)),
        "prior_down_grad": heavy_noise(key_list[6], (N_DP, LAYERS, FF, D), 1.0, 6.0, ((0, 32), (1, 4), (2, 2)), (0, 2, 32, 2.75)),
        "master_up": centred(key_list[7], (LAYERS, D, FF), 0.05, 0.3, ((0, 4), (1, 32), (2, 2)), jnp.float32),
        "master_down": centred(key_list[8], (LAYERS, FF, D), 0.05, 0.3, ((0, 4), (1, 64)), jnp.float32),
    }


eps_norm = 1e-05
gelu_coef = 0.7978845608028654
learning_rate = 0.05

def gelu_tanh(value):
    inner = jnp.tanh(gelu_coef * (value + 0.044715 * value * value * value))
    return 0.5 * value * (1.0 + inner)

def gelu_slope(value):
    inner = jnp.tanh(gelu_coef * (value + 0.044715 * value * value * value))
    return 0.5 * (1.0 + inner) + 0.5 * value * (1.0 - inner * inner) * gelu_coef * (1.0 + 3.0 * 0.044715 * value * value)

def apply_norm(layer_entry_input, gain_vector):
    values = layer_entry_input.astype(jnp.float32)
    center = lax.optimization_barrier(jnp.mean(values, axis=-1, keepdims=True))
    centered_rows = values - center
    spread = lax.optimization_barrier(jnp.mean(centered_rows * centered_rows, axis=-1, keepdims=True))
    inverse_scale = lax.rsqrt(spread + eps_norm)
    standardized_input = centered_rows * inverse_scale
    return ((standardized_input * gain_vector).astype(jnp.bfloat16), standardized_input, inverse_scale)

def layer_forward(layer_entry_input, gain_vector, w_up, w_down):
    normalized_rows, standardized_input, inverse_scale = apply_norm(layer_entry_input, gain_vector)
    upper = jnp.dot(normalized_rows, w_up, preferred_element_type=jnp.float32)
    active = gelu_tanh(upper).astype(jnp.bfloat16)
    mixed = jnp.dot(active, w_down, preferred_element_type=jnp.float32)
    return (layer_entry_input.astype(jnp.float32) + mixed).astype(jnp.bfloat16)

def layer_backward(layer_entry_input, upstream_gradient, gain_vector, w_up, w_down):
    normalized_rows, standardized_input, inverse_scale = apply_norm(layer_entry_input, gain_vector)
    upper = jnp.dot(normalized_rows, w_up, preferred_element_type=jnp.float32)
    grad_act = jnp.dot(upstream_gradient, w_down.T, preferred_element_type=jnp.float32)
    grad_up = (grad_act * gelu_slope(upper)).astype(jnp.bfloat16)
    normalized_gradient = jnp.dot(grad_up, w_up.T, preferred_element_type=jnp.float32)
    rescaled_rows = normalized_gradient * gain_vector
    leading_operand = lax.optimization_barrier(jnp.mean(rescaled_rows, axis=-1, keepdims=True))
    trailing_operand = lax.optimization_barrier(jnp.mean(rescaled_rows * standardized_input, axis=-1, keepdims=True))
    final_output = upstream_gradient.astype(jnp.float32) + inverse_scale * (rescaled_rows - leading_operand - standardized_input * trailing_operand)
    return final_output.astype(jnp.bfloat16)

def reference(inputs, out_grads, norm_gain, up_weight, down_weight, prior_up_grad, prior_down_grad, master_up, master_down):
    outputs_all = []
    stored_inputs = []
    for layer in range(LAYERS):
        outputs_row = []
        inputs_row = []
        for micro in range(MICRO):
            current = inputs[micro] if layer == 0 else outputs_all[layer - 1][micro]
            inputs_row.append(current)
            outputs_row.append(layer_forward(current, norm_gain[layer], up_weight[layer], down_weight[layer]))
        outputs_all.append(outputs_row)
        stored_inputs.append(inputs_row)
    grads_all = [None] * LAYERS
    for layer in range(LAYERS - 1, -1, -1):
        grads_row = []
        for micro in range(MICRO):
            upstream_gradient = out_grads[micro] if layer == LAYERS - 1 else grads_all[layer + 1][micro]
            grads_row.append(layer_backward(stored_inputs[layer][micro], upstream_gradient, norm_gain[layer], up_weight[layer], down_weight[layer]))
        grads_all[layer] = grads_row
    layer_outputs = jnp.stack([jnp.stack(row) for row in outputs_all])
    input_grads = jnp.stack([jnp.stack(row) for row in grads_all])
    up_total = lax.optimization_barrier(jnp.sum(prior_up_grad.astype(jnp.float32), axis=0))
    down_total = lax.optimization_barrier(jnp.sum(prior_down_grad.astype(jnp.float32), axis=0))
    new_up = master_up - learning_rate * up_total
    new_down = master_down - learning_rate * down_total
    return (layer_outputs, input_grads, new_up, new_down)
```

```python
import jax
import jax.numpy as jnp
from jax import lax
from jax.sharding import PartitionSpec as P

eps_norm = 1e-05
gelu_coef = 0.7978845608028654
learning_rate = 0.05
bf16 = jnp.bfloat16
f32 = jnp.float32
side = 4
cores = 2


def hand_over(value, source, target, sections):
    axes = ("section", "tensor")
    halves = lax.axis_size("tensor")
    straight = lax.ppermute(
        value, axes, [(source * halves + t, target * halves + t) for t in range(halves)]
    )
    crossed = lax.ppermute(
        value, axes, [(source * halves + t, target * halves + 1 - t) for t in range(halves)]
    )
    return (straight.astype(f32) + crossed.astype(f32)).astype(bf16)


def with_other_half(value):
    other = lax.ppermute(value, "tensor", [(0, 1), (1, 0)])
    return (value.astype(f32) + other.astype(f32)).astype(bf16)


def apply_norm(rows, gain):
    values = rows.astype(f32)
    center = jnp.mean(values, axis=-1, keepdims=True)
    centered = values - center
    spread = jnp.mean(centered * centered, axis=-1, keepdims=True)
    inverse_scale = lax.rsqrt(spread + eps_norm)
    return centered * inverse_scale, inverse_scale


def forward_part(rows, gain, w_up, w_down):
    standardized, _ = apply_norm(rows, gain)
    upper = jnp.dot((standardized * gain).astype(bf16), w_up, preferred_element_type=f32)
    inner = jnp.tanh(gelu_coef * (upper + 0.044715 * upper * upper * upper))
    active = (0.5 * upper * (1.0 + inner)).astype(bf16)
    part = jnp.dot(active, w_down, preferred_element_type=f32)
    return (part + 0.5 * rows.astype(f32)).astype(bf16)


def slope_of(rows, gain, w_up):
    standardized, inverse_scale = apply_norm(rows, gain)
    upper = jnp.dot((standardized * gain).astype(bf16), w_up, preferred_element_type=f32)
    inner = jnp.tanh(gelu_coef * (upper + 0.044715 * upper * upper * upper))
    slope = 0.5 * (1.0 + inner) + 0.5 * upper * (1.0 - inner * inner) * gelu_coef * (
        1.0 + 3.0 * 0.044715 * upper * upper
    )
    return slope, standardized, inverse_scale


def backward_part(grad, slope, standardized, inverse_scale, gain, w_up, w_down):
    across = (((1,), (1,)), ((), ()))
    grad_act = lax.dot_general(grad, w_down, across, preferred_element_type=f32)
    grad_up = (grad_act * slope).astype(bf16)
    part = lax.dot_general(grad_up, w_up, across, preferred_element_type=f32) * gain
    leading = jnp.mean(part, axis=-1, keepdims=True)
    trailing = jnp.mean(part * standardized, axis=-1, keepdims=True)
    moved = inverse_scale * (part - leading - standardized * trailing)
    return (moved + 0.5 * grad.astype(f32)).astype(bf16)


def by_position(axis, move):
    pairs = []
    for x in range(side):
        for y in range(side):
            for core in range(cores):
                place = [x, y, core]
                place[axis] = move(place[axis])
                pairs.append(((x * side + y) * cores + core, (place[0] * side + place[1]) * cores + place[2]))
    return pairs


def near(position):
    return position ^ 1


def wrapped(position):
    return side - 1 - position


def block(value, index):
    return lax.dynamic_index_in_dim(value, index, 0, keepdims=False)


def plus(a, b):
    return (a.astype(f32) + b.astype(f32)).astype(bf16)


def line_sum(value, axis, position, first, second):
    there = first(position)
    sent = jnp.stack([block(value, there), block(value, second(there))])
    got = lax.ppermute(sent, "dp", by_position(axis, first))
    kept = plus(block(value, second(position)), got[1])
    mine = plus(block(value, position), got[0])
    return plus(mine, lax.ppermute(kept, "dp", by_position(axis, second)))


def summed_shards(up, down):
    index = lax.axis_index("dp")
    core, y, x = index % cores, (index // cores) % side, index // (cores * side)
    totals = []
    for value, order in ((up, ((0, x), (1, y))), (down, ((1, y), (0, x)))):
        rows = value.shape[0] // (side * side * cores)
        value = value.reshape(side, side, cores, rows, value.shape[1])
        own = lax.dynamic_index_in_dim(value, core, 2, keepdims=False)
        other = lax.dynamic_index_in_dim(value, 1 - core, 2, keepdims=False)
        value = plus(own, lax.ppermute(other, "dp", by_position(2, lambda c: 1 - c)))
        if order[0][0] == 1:
            value = jnp.swapaxes(value, 0, 1)
        parts = []
        half = rows // 2
        for at, moves in ((0, (near, wrapped)), (half, (wrapped, near))):
            part = value[:, :, at : at + half]
            for axis, position in order:
                part = line_sum(part, axis, position, *moves)
            parts.append(part)
        totals.append(jnp.concatenate(parts, axis=0))
    return totals


def local(
    inputs,
    out_grads,
    norm_gain,
    up_weight,
    down_weight,
    prior_up_grad,
    prior_down_grad,
    master_up,
    master_down,
):
    up_total, down_total = summed_shards(prior_up_grad[0, 0], prior_down_grad[0, 0])
    new_up = master_up - learning_rate * up_total.astype(f32)[None]
    new_down = master_down - learning_rate * down_total.astype(f32)[None]

    sections = lax.axis_size("section")
    section = lax.axis_index("section")
    width = inputs.shape[-1]
    gain = norm_gain[0]
    w_up = up_weight[0]
    w_down = down_weight[0]
    rows = inputs.reshape(-1, width)
    for stage in range(sections - 1):
        part = forward_part(rows, gain, w_up, w_down)
        rows = jnp.where(section == stage + 1, hand_over(part, stage, stage + 1, sections), rows)
    produced = with_other_half(forward_part(rows, gain, w_up, w_down))
    slope, standardized, inverse_scale = slope_of(rows, gain, w_up)
    grad = out_grads.reshape(-1, width)
    for stage in range(sections - 1, 0, -1):
        part = backward_part(grad, slope, standardized, inverse_scale, gain, w_up, w_down)
        grad = jnp.where(section == stage - 1, hand_over(part, stage, stage - 1, sections), grad)
    part = backward_part(grad, slope, standardized, inverse_scale, gain, w_up, w_down)
    grads_done = with_other_half(part)
    shape = (1, *inputs.shape)
    return (produced.reshape(shape), grads_done.reshape(shape), new_up, new_down)


def solution(mesh):
    placed = (
        P(None, "dp", None),
        P(None, "dp", None),
        P("section", None),
        P("section", None, "tensor"),
        P("section", "tensor", None),
        P("dp", "section", None, "tensor"),
        P("dp", "section", "tensor", None),
        P("section", "dp", "tensor"),
        P("section", ("tensor", "dp"), None),
    )
    return jax.shard_map(
        local,
        mesh=mesh,
        in_specs=placed,
        out_specs=(
            P("section", None, "dp", None),
            P("section", None, "dp", None),
            P("section", "dp", "tensor"),
            P("section", ("tensor", "dp"), None),
        ),
        check_vma=False,
    )
```

```python
from functools import partial

import jax
import jax.numpy as jnp
from jax import lax
from jax.experimental import pallas as pl
from jax.experimental.pallas import tpu as pltpu
from jax.sharding import PartitionSpec as P


eps_norm = 1e-05
gelu_coef = 0.7978845608028654
learning_rate = 0.05
bf16 = jnp.bfloat16
f32 = jnp.float32
side = 4
cores = 2


def hand_over(value, source, target):
    axes = ("section", "tensor")
    halves = lax.axis_size("tensor")
    straight = lax.ppermute(
        value, axes, [(source * halves + t, target * halves + t) for t in range(halves)]
    )
    crossed = lax.ppermute(
        value, axes, [(source * halves + t, target * halves + 1 - t) for t in range(halves)]
    )
    return straight, crossed


def handed(value, moves):
    halves = lax.axis_size("tensor")
    return lax.ppermute(
        value, ("section", "tensor"), [(a * halves + t, b * halves + u) for (a, t), (b, u) in moves]
    )


chunk = 512


def apply_norm(values):
    center = jnp.mean(values, axis=-1, keepdims=True)
    centered = values - center
    spread = jnp.mean(centered * centered, axis=-1, keepdims=True)
    inverse_scale = lax.rsqrt(spread + eps_norm)
    return centered * inverse_scale, inverse_scale


def plus(a, b):
    return (a.astype(f32) + b.astype(f32)).astype(bf16)


def chosen(stage, straight, crossed, kept):
    return jnp.where(lax.axis_index("section") == stage, plus(straight[...], crossed[...]), kept[...])


def up_of(normed, w_up, at):
    return jnp.dot(normed, w_up[:, at : at + chunk], preferred_element_type=f32)


def curve(upper):
    square = upper * upper
    return jnp.tanh(gelu_coef * (upper + 0.044715 * square * upper)), square


def down_part(rows, act, w_down):
    part = jnp.dot(act[...], w_down[...], preferred_element_type=f32)
    return (part + 0.5 * rows.astype(f32)).astype(bf16)


def forward_body(stage, straight, crossed, kept, gain, w_up, w_down, rows_out, part_out, act):
    rows = chosen(stage, straight, crossed, kept)
    rows_out[...] = rows
    standardized, _ = apply_norm(rows.astype(f32))
    normed = (standardized * gain[...]).astype(bf16)
    for at in range(0, act.shape[1], chunk):
        upper = up_of(normed, w_up, at)
        inner, _ = curve(upper)
        act[:, at : at + chunk] = (0.5 * upper * (1.0 + inner)).astype(bf16)
    part_out[...] = down_part(rows, act, w_down)


def first_body(kept, gain, w_up, w_down, part_out, up_here, down_here, act, came):
    hidden = act.shape[1]
    loads = []
    for i, at in enumerate(range(0, hidden, chunk)):
        here = pl.ds(at, chunk)
        loads.append(pltpu.make_async_copy(w_up.at[:, here], up_here.at[:, here], came.at[i]))
    loads.append(pltpu.make_async_copy(w_down, down_here, came.at[len(loads)]))
    for load in loads:
        load.start()
    rows = kept[...]
    standardized, _ = apply_norm(rows.astype(f32))
    normed = (standardized * gain[...]).astype(bf16)
    for i, at in enumerate(range(0, hidden, chunk)):
        loads[i].wait()
        upper = up_of(normed, up_here, at)
        inner, _ = curve(upper)
        act[:, at : at + chunk] = (0.5 * upper * (1.0 + inner)).astype(bf16)
    loads[-1].wait()
    part_out[...] = down_part(rows, act, down_here)


def grad_part(grad, pushed, standardized, inverse_scale, gain, w_up):
    part = lax.dot_general(pushed[...], w_up[...], across, preferred_element_type=f32) * gain
    leading = jnp.mean(part, axis=-1, keepdims=True)
    trailing = jnp.mean(part * standardized, axis=-1, keepdims=True)
    moved = inverse_scale * (part - leading - standardized * trailing)
    return (moved + 0.5 * grad.astype(f32)).astype(bf16)


across = (((1,), (1,)), ((), ()))


def turn_body(stage, straight, crossed, kept, grad_in, gain, w_up, w_down, rows_out, act, slope, part_out, pushed):
    rows = chosen(stage, straight, crossed, kept)
    rows_out[...] = rows
    standardized, inverse_scale = apply_norm(rows.astype(f32))
    normed = (standardized * gain[...]).astype(bf16)
    grad = grad_in[...]
    for at in range(0, act.shape[1], chunk):
        here = slice(at, at + chunk)
        upper = up_of(normed, w_up, at)
        inner, square = curve(upper)
        act[:, here] = (0.5 * upper * (1.0 + inner)).astype(bf16)
        rise = 0.5 * (1.0 + inner) + 0.5 * upper * (1.0 - inner * inner) * gelu_coef * (
            1.0 + 3.0 * 0.044715 * square
        )
        slope[:, here] = rise
        grad_act = lax.dot_general(grad, w_down[here, :], across, preferred_element_type=f32)
        pushed[:, here] = (grad_act * rise).astype(bf16)
    part_out[...] = grad_part(grad, pushed, standardized, inverse_scale, gain[...], w_up)


def mix_body(last, rows, act, w_down, part_out):
    part = down_part(rows[...], act, w_down)
    part_out[...] = jnp.where(lax.axis_index("section") == last, part, rows[...])


def produced_body(last, mixed, back, swapped, out):
    section = lax.axis_index("section")
    other = jnp.where(section == last - 1, swapped[...], back[...])
    out[...] = jnp.where(section == last, plus(mixed[...], back[...]), other)


def grads_body(part, other, swapped, *rest):
    *backs, out = rest
    section = lax.axis_index("section")
    value = swapped[...]
    for at, back in enumerate(backs):
        value = jnp.where(section == at + 1, back[...], value)
    out[...] = jnp.where(section == 0, plus(part[...], other[...]), value)


def backward_body(stage, last, straight, crossed, kept, rows, slope, gain, w_up, w_down, grad_out, part_out, *more):
    *swap_out, pushed = more
    grad = chosen(stage, straight, crossed, kept)
    grad_out[...] = grad
    if swap_out:
        swap_out[0][...] = jnp.where(lax.axis_index("section") == last, rows[...], grad)
    for at in range(0, pushed.shape[1], chunk):
        here = slice(at, at + chunk)
        grad_act = lax.dot_general(grad, w_down[here, :], across, preferred_element_type=f32)
        pushed[:, here] = (grad_act * slope[:, here]).astype(bf16)
    standardized, inverse_scale = apply_norm(rows[...].astype(f32))
    part_out[...] = grad_part(grad, pushed, standardized, inverse_scale, gain[...], w_up)


def held(*arrays):
    return [(array, "held") for array in arrays]


def kernel(body, outs, operands, scratch=(), plain=False):
    spaces = {"held": pltpu.VMEM, "copied": pltpu.VMEM, "far": pltpu.HBM}
    in_vmem = pl.BlockSpec(memory_space=pltpu.VMEM)
    return pl.pallas_call(
        body,
        out_shape=[(jax.ShapeDtypeStruct if plain else pltpu.VMEM)(shape, dtype) for shape, dtype in outs],
        in_specs=[pl.BlockSpec(memory_space=spaces[where]) for _, where in operands],
        out_specs=[in_vmem] * len(outs),
        scratch_shapes=list(scratch),
        compiler_params=pltpu.CompilerParams(vmem_limit_bytes=16 * 2**20),
    )(
        *(
            pltpu.with_memory_space_constraint(array, spaces[where]) if where in ("held", "far") else array
            for array, where in operands
        )
    )


def by_position(axis, move):
    pairs = []
    for x in range(side):
        for y in range(side):
            for core in range(cores):
                place = [x, y, core]
                place[axis] = move(place[axis])
                pairs.append(((x * side + y) * cores + core, (place[0] * side + place[1]) * cores + place[2]))
    return pairs


def near(position):
    return position ^ 1


def wrapped(position):
    return side - 1 - position


def after(values, event):
    return lax.optimization_barrier((values, event))[0]


def my_core():
    return lax.rem(lax.axis_index("dp"), cores)


def my_places(axis):
    chip = lax.div(lax.axis_index("dp"), cores)
    own = lax.rem(chip, side) if axis else lax.div(chip, side)
    beside = near(own)
    return own, wrapped(own), beside, wrapped(beside)


def split_body(up, down, own, other, came):
    mine = my_core()
    rows, columns = up.shape[3], own.shape[-1]
    copies = []
    for to, core in ((own, mine), (other, cores - 1 - mine)):
        for part in range(up.shape[4] // columns):
            source = up.at[:, :, core, :, pl.ds(part * columns, columns)]
            copies.append((source, to.at[0, :, :, pl.ds(part * rows, rows), :]))
        copies.append((down.at[:, :, core], to.at[1]))
    copies = [pltpu.make_async_copy(a, b, came.at[i]) for i, (a, b) in enumerate(copies)]
    for copy in copies:
        copy.start()
    for copy in copies:
        copy.wait()


def halved_body(own, got, up_kept, up_sent, down_kept, down_sent):
    places = my_places(0), my_places(1)
    for line in range(side):
        for at, (kept, sent) in enumerate(((up_kept, up_sent), (down_kept, down_sent))):
            for slot in range(4):
                place = places[at][slot]
                block = (at, place, line) if at == 0 else (at, line, place)
                to = kept if slot < 2 else sent
                to[slot % 2, line] = plus(own[block], got[block])


def paired_body(up_kept, up_got, down_kept, down_got, up_mine, up_sent, down_mine, down_sent):
    for kept, got, mine, sent in ((up_kept, up_got, up_mine, up_sent), (down_kept, down_got, down_mine, down_sent)):
        mine[...] = plus(kept[0], got[0])
        sent[...] = plus(kept[1], got[1])


def crossing_body(up_mine, up_got, down_mine, down_got, up_kept, up_sent, down_kept, down_sent):
    places = my_places(1), my_places(0)
    for at, (mine, got, kept, sent) in enumerate(
        ((up_mine, up_got, up_kept, up_sent), (down_mine, down_got, down_kept, down_sent))
    ):
        for slot in range(4):
            place = places[at][slot]
            to = kept if slot < 2 else sent
            to[slot % 2] = plus(mine[place], got[place])


def settled_body(up_mine, up_got, down_mine, down_got, master_up, master_down, new_up, new_down):
    rows, columns = master_up.shape[0], up_mine.shape[1]
    for part in range(master_up.shape[1] // columns):
        here, there = slice(part * rows, (part + 1) * rows), slice(part * columns, (part + 1) * columns)
        total = up_mine[here, :].astype(f32) + up_got[here, :].astype(f32)
        new_up[:, there] = master_up[:, there] - learning_rate * total
    total = down_mine[...].astype(f32) + down_got[...].astype(f32)
    new_down[...] = master_down[...] - learning_rate * total


def local(
    inputs,
    out_grads,
    norm_gain,
    up_weight,
    down_weight,
    prior_up_grad,
    prior_down_grad,
    master_up,
    master_down,
):
    turn = 0

    def move(part, source, target):
        fresh = hand_over(part, source, target)
        return summing(part, fresh)

    columns = down_weight.shape[2]
    shape = (down_weight.shape[1] // (side * side * cores), columns)
    whole, pair, line, two = (2, side, side, *shape), (2, side, *shape), (side, *shape), (2, *shape)
    axes = ((0, 1), (1, 0))
    state, gots = None, None

    def summing(event, arrivals):
        nonlocal turn, state, gots
        if turn == 0:
            up = prior_up_grad.reshape(side, side, cores, -1, prior_up_grad.shape[-1])
            down = prior_down_grad.reshape(side, side, cores, *shape)
            loads = pltpu.SemaphoreType.DMA((2 * (up.shape[-1] // columns + 1),))
            up, down = after((up, down), event)
            own, other = kernel(split_body, [(whole, bf16)] * 2, [(up, "far"), (down, "far")], [loads])
            gate = other
            state = [own]
            gots = [lax.ppermute(other, "dp", by_position(2, lambda c: 1 - c))]
        else:
            read = [array for both in zip(state, gots) for array in both]
            read = held(*after(read, event))
            if turn == 1:
                made = kernel(halved_body, [(pair, bf16)] * 4, read)
            elif turn == 2:
                made = kernel(paired_body, [(line, bf16)] * 4, read)
            elif turn == 3:
                made = kernel(crossing_body, [(two, bf16)] * 4, read)
            elif turn == 4:
                made = kernel(paired_body, [(shape, bf16)] * 4, read)
            else:
                masters = [(master_up[0], "copied"), (master_down[0], "copied")]
                outs = [(master_up.shape[1:], f32), (master_down.shape[1:], f32)]
                made = kernel(settled_body, outs, [*read, *masters], plain=True)
            gate = made
            if turn < 5:
                state = [made[0], made[2]]
                moved = near if turn % 2 else wrapped
                gots = [
                    lax.ppermute(made[2 * at + 1], "dp", by_position(axes[at][(turn - 1) // 2], moved))
                    for at in range(2)
                ]
            else:
                state = made
        turn += 1
        return after(arrivals, gate)

    sections = lax.axis_size("section")
    last, both = sections - 1, range(lax.axis_size("tensor"))
    width = inputs.shape[-1]
    gain, w_up, w_down = norm_gain, up_weight[0], down_weight[0]
    rows, grad = inputs.reshape(-1, width), out_grads.reshape(-1, width)
    count, hidden = rows.shape[0], w_up.shape[1]
    narrow, wide, broad = ((count, width), bf16), ((count, hidden), bf16), ((count, hidden), f32)
    scratch = [pltpu.VMEM((count, hidden), bf16)]
    loads = pltpu.SemaphoreType.DMA((hidden // chunk + 1,))
    part, up_here, down_here = kernel(
        first_body,
        [narrow, (w_up.shape, bf16), (w_down.shape, bf16)],
        [(rows, "copied"), (gain, "copied"), (w_up, "far"), (w_down, "far")],
        [*scratch, loads],
    )
    weights = [(gain, "copied"), *held(up_here, down_here)]
    kept = (rows, "copied")

    for stage in range(1, last):
        fresh = move(part, stage - 1, stage)
        rows, part = kernel(partial(forward_body, stage), [narrow, narrow], [*held(*fresh), kept, *weights], scratch)
        kept = (rows, "held")
    fresh = move(part, last - 1, last)
    rows, act, slope, part = kernel(
        partial(turn_body, last),
        [narrow, wide, broad, narrow],
        [*held(*fresh), kept, (grad, "copied"), *weights],
        scratch,
    )
    kept = (grad, "copied")
    backs = []
    for stage in range(last - 1, -1, -1):
        fresh = move(part, stage + 1, stage)
        if stage == last - 1:
            (mixed,) = kernel(partial(mix_body, last), [narrow], held(rows, act, down_here))
            back = handed(
                mixed,
                [((last, t), (last, 1 - t)) for t in both]
                + [((s + 1, t), (s, t)) for s in range(last - 1) for t in both],
            )
        grad, part, *swap = kernel(
            partial(backward_body, stage, last),
            [narrow] * (3 if stage == last - 1 else 2),
            [*held(*fresh), kept, *held(rows, slope), *weights],
            scratch,
        )
        kept = (grad, "held")
        if swap:
            swapped = handed(
                swap[0],
                [((last, t), (last - 1, t)) for t in both] + [((last - 1, 1 - t), (last, t)) for t in both],
            )
        else:
            backs.append(handed(grad, [((stage, 1 - t), (stage + 1, t)) for t in both]))
    other = handed(part, [((0, t), (0, 1 - t)) for t in both])
    (produced,) = kernel(partial(produced_body, last), [narrow], held(mixed, back, swapped), plain=True)
    (grads_done,) = kernel(grads_body, [narrow], held(part, other, swapped, *backs[::-1]), plain=True)
    new_up, new_down = state[0][None], state[1][None]
    shape = (1, *inputs.shape)
    return (produced.reshape(shape), grads_done.reshape(shape), new_up, new_down)


def solution(mesh):
    placed = (
        P(None, "dp", None),
        P(None, "dp", None),
        P("section", None),
        P("section", None, "tensor"),
        P("section", "tensor", None),
        P("dp", "section", None, "tensor"),
        P("dp", "section", "tensor", None),
        P("section", "dp", "tensor"),
        P("section", ("tensor", "dp"), None),
    )
    return jax.shard_map(
        local,
        mesh=mesh,
        in_specs=placed,
        out_specs=(
            P("section", None, "dp", None),
            P("section", None, "dp", None),
            P("section", "dp", "tensor"),
            P("section", ("tensor", "dp"), None),
        ),
        check_vma=False,
    )
```

```python
from functools import partial

import jax
import jax.numpy as jnp
from jax import lax
from jax.experimental import pallas as pl
from jax.experimental.pallas import tpu as pltpu
from jax.sharding import PartitionSpec as P


eps_norm = 1e-05
gelu_coef = 0.7978845608028654
learning_rate = 0.05
bf16 = jnp.bfloat16
f32 = jnp.float32
side = 4
cores = 2


def hand_over(value, source, target):
    both = range(lax.axis_size("tensor"))
    crossed = handed(value, [((source, t), (target, 1 - t)) for t in both])
    straight = handed(value, [((source, t), (target, t)) for t in both])
    return straight, crossed


def handed(value, moves):
    halves = lax.axis_size("tensor")
    return lax.ppermute(
        value, ("section", "tensor"), [(a * halves + t, b * halves + u) for (a, t), (b, u) in moves]
    )


chunk = 512


def apply_norm(values):
    center = jnp.mean(values, axis=-1, keepdims=True)
    centered = values - center
    spread = jnp.mean(centered * centered, axis=-1, keepdims=True)
    inverse_scale = lax.rsqrt(spread + eps_norm)
    return centered * inverse_scale, inverse_scale


def plus(a, b):
    return (a.astype(f32) + b.astype(f32)).astype(bf16)


def chosen(stage, straight, crossed, kept):
    return jnp.where(lax.axis_index("section") == stage, plus(straight[...], crossed[...]), kept)


def up_of(normed, w_up, at):
    return jnp.dot(normed, w_up[:, at : at + chunk], preferred_element_type=f32)


def curve(upper):
    square = upper * upper
    return jnp.tanh(gelu_coef * (upper + 0.044715 * square * upper)), square


def rows_of(array, micro):
    return array[micro] if len(array.shape) == 3 else array[...]


def down_part(rows, act, w_down):
    part = jnp.dot(act[...], w_down[...], preferred_element_type=f32)
    return (part + 0.5 * rows.astype(f32)).astype(bf16)


def activate(rows, gain, w_up, act, ready=None):
    standardized, _ = apply_norm(rows.astype(f32))
    normed = (standardized * gain[...]).astype(bf16)
    for i, at in enumerate(range(0, act.shape[1], chunk)):
        if ready:
            ready[i].wait()
        upper = up_of(normed, w_up, at)
        inner, _ = curve(upper)
        act[:, at : at + chunk] = (0.5 * upper * (1.0 + inner)).astype(bf16)


def first_body(inputs, gain, w_up, w_down, part_out, inputs_here, gain_here, up_here, down_here, act, came):
    pairs = [(inputs, inputs_here), (gain, gain_here)]
    for at in range(0, act.shape[1], chunk):
        here = pl.ds(at, chunk)
        pairs.append((w_up.at[:, here], up_here.at[:, here]))
    pairs.append((w_down, down_here))
    loads = [pltpu.make_async_copy(a, b, came.at[i]) for i, (a, b) in enumerate(pairs)]
    for load in loads:
        load.start()
    loads[0].wait()
    loads[1].wait()
    rows = inputs_here[0]
    activate(rows, gain_here, up_here, act, loads[2:-1])
    loads[-1].wait()
    part_out[...] = down_part(rows, act, down_here)


def at_section(stage):
    return pl.when(lax.axis_index("section") == stage)


def opening_body(micro, inputs, gain, w_up, w_down, part_out, act):
    @at_section(0)
    def _():
        rows = inputs[micro]
        activate(rows, gain, w_up, act)
        part_out[...] = down_part(rows, act, w_down)


def forward_body(stage, micro, straight, crossed, kept, gain, w_up, w_down, rows_out, part_out, act):
    rows = chosen(stage, straight, crossed, rows_of(kept, micro))
    rows_out[...] = rows

    @at_section(stage)
    def _():
        activate(rows, gain, w_up, act)
        part_out[...] = down_part(rows, act, w_down)


def grad_part(grad, pushed, standardized, inverse_scale, gain, w_up):
    part = lax.dot_general(pushed[...], w_up[...], across, preferred_element_type=f32) * gain
    leading = jnp.mean(part, axis=-1, keepdims=True)
    trailing = jnp.mean(part * standardized, axis=-1, keepdims=True)
    moved = inverse_scale * (part - leading - standardized * trailing)
    return (moved + 0.5 * grad.astype(f32)).astype(bf16)


across = (((1,), (1,)), ((), ()))


def slope_of(upper, inner, square):
    return 0.5 * (1.0 + inner) + 0.5 * upper * (1.0 - inner * inner) * gelu_coef * (1.0 + 3.0 * 0.044715 * square)


def turn_body(stage, micro, straight, crossed, kept, grad_in, gain, w_up, w_down, rows_out, act, part_out, pushed):
    rows = chosen(stage, straight, crossed, rows_of(kept, micro))
    rows_out[...] = rows

    @at_section(stage)
    def _():
        standardized, inverse_scale = apply_norm(rows.astype(f32))
        normed = (standardized * gain[...]).astype(bf16)
        grad = grad_in[micro]
        for at in range(0, act.shape[1], chunk):
            here = slice(at, at + chunk)
            upper = up_of(normed, w_up, at)
            inner, square = curve(upper)
            act[:, here] = (0.5 * upper * (1.0 + inner)).astype(bf16)
            grad_act = lax.dot_general(grad, w_down[here, :], across, preferred_element_type=f32)
            pushed[:, here] = (grad_act * slope_of(upper, inner, square)).astype(bf16)
        part_out[...] = grad_part(grad, pushed, standardized, inverse_scale, gain[...], w_up)


def slope_body(last, *refs):
    count = (len(refs) - 2) // 2
    gain, w_up = refs[count : count + 2]

    @pl.when(lax.axis_index("section") < last)
    def _():
        for rows, slope in zip(refs[:count], refs[count + 2 :]):
            standardized, _ = apply_norm(rows[...].astype(f32))
            normed = (standardized * gain[...]).astype(bf16)
            for at in range(0, slope.shape[1], chunk):
                upper = up_of(normed, w_up, at)
                inner, square = curve(upper)
                slope[:, at : at + chunk] = slope_of(upper, inner, square)


def backward_body(stage, micro, straight, crossed, kept, rows, slope, gain, w_up, w_down, grad_out, part_out, pushed):
    grad = chosen(stage, straight, crossed, rows_of(kept, micro))
    grad_out[...] = grad

    @at_section(stage)
    def _():
        for at in range(0, pushed.shape[1], chunk):
            here = slice(at, at + chunk)
            grad_act = lax.dot_general(grad, w_down[here, :], across, preferred_element_type=f32)
            pushed[:, here] = (grad_act * slope[:, here]).astype(bf16)
        standardized, inverse_scale = apply_norm(rows[...].astype(f32))
        part_out[...] = grad_part(grad, pushed, standardized, inverse_scale, gain[...], w_up)


def stacked(parts):
    return jnp.concatenate([part[...] for part in parts], axis=0)


def mix_body(last, *refs):
    *pairs, w_down, out = refs
    count = pairs[0].shape[0]

    @at_section(last)
    def _():
        for at in range(len(pairs) // 2):
            out[at * count : (at + 1) * count, :] = down_part(pairs[2 * at][...], pairs[2 * at + 1], w_down)


def pack_body(*refs):
    *parts, out = refs
    out[...] = stacked(parts)


def produced_body(mixed, other, *refs):
    *backs, out = refs
    section = lax.axis_index("section")
    value = plus(mixed[...], other[...])
    for at, back in enumerate(backs):
        value = jnp.where(section == at, back[...], value)
    out[...] = value


def grads_body(micros, early, late, *refs):
    *ends, out = refs
    section = lax.axis_index("section")
    mine = jnp.concatenate([plus(ends[2 * at][...], ends[2 * at + 1][...]) for at in range(micros)], axis=0)
    back = jnp.where(lax.rem(section, 2) == 1, late[...], early[...])
    out[...] = jnp.where(section == 0, mine, back)


def held(*arrays):
    return [(array, "held") for array in arrays]


def kernel(body, outs, operands, scratch=(), plain=False):
    spaces = {"held": pltpu.VMEM, "copied": pltpu.VMEM, "far": pltpu.HBM}
    in_vmem = pl.BlockSpec(memory_space=pltpu.VMEM)
    return pl.pallas_call(
        body,
        out_shape=[(jax.ShapeDtypeStruct if plain else pltpu.VMEM)(shape, dtype) for shape, dtype in outs],
        in_specs=[pl.BlockSpec(memory_space=spaces[where]) for _, where in operands],
        out_specs=[in_vmem] * len(outs),
        scratch_shapes=list(scratch),
        compiler_params=pltpu.CompilerParams(vmem_limit_bytes=16 * 2**20),
    )(
        *(
            pltpu.with_memory_space_constraint(array, spaces[where]) if where in ("held", "far") else array
            for array, where in operands
        )
    )


def by_position(axis, move):
    pairs = []
    for x in range(side):
        for y in range(side):
            for core in range(cores):
                place = [x, y, core]
                place[axis] = move(place[axis])
                pairs.append(((x * side + y) * cores + core, (place[0] * side + place[1]) * cores + place[2]))
    return pairs


def near(position):
    return position ^ 1


def wrapped(position):
    return side - 1 - position


def my_core():
    return lax.rem(lax.axis_index("dp"), cores)


def my_places(axis):
    chip = lax.div(lax.axis_index("dp"), cores)
    own = lax.rem(chip, side) if axis else lax.div(chip, side)
    beside = near(own)
    return own, wrapped(own), beside, wrapped(beside)


def split_body(up, down, own, other, came):
    mine = my_core()
    rows, columns = up.shape[3], own.shape[-1]
    copies = []
    for to, core in ((own, mine), (other, cores - 1 - mine)):
        for part in range(up.shape[4] // columns):
            source = up.at[:, :, core, :, pl.ds(part * columns, columns)]
            copies.append((source, to.at[0, :, :, pl.ds(part * rows, rows), :]))
        copies.append((down.at[:, :, core], to.at[1]))
    copies = [pltpu.make_async_copy(a, b, came.at[i]) for i, (a, b) in enumerate(copies)]
    for copy in copies:
        copy.start()
    for copy in copies:
        copy.wait()


def halved_body(own, got, kept, sent):
    places = my_places(0)
    for slot in range(4):
        to = kept if slot < 2 else sent
        for weight in range(2):
            for line in range(side):
                block = (weight, places[slot], line)
                to[slot % 2, weight, line] = plus(own[block], got[block])


def paired_body(kept, got, mine, sent):
    mine[...] = plus(kept[0], got[0])
    sent[...] = plus(kept[1], got[1])


def crossing_body(mine, got, kept, sent):
    places = my_places(1)
    for slot in range(4):
        to = kept if slot < 2 else sent
        for weight in range(2):
            block = (weight, places[slot])
            to[slot % 2, weight] = plus(mine[block], got[block])


def settled_body(mine, got, master_up, master_down, new_up, new_down):
    rows, columns = master_up.shape[0], mine.shape[2]
    for part in range(master_up.shape[1] // columns):
        here, there = slice(part * rows, (part + 1) * rows), slice(part * columns, (part + 1) * columns)
        total = mine[0, here, :].astype(f32) + got[0, here, :].astype(f32)
        new_up[:, there] = master_up[:, there] - learning_rate * total
    total = mine[1].astype(f32) + got[1].astype(f32)
    new_down[...] = master_down[...] - learning_rate * total


def local(
    inputs,
    out_grads,
    norm_gain,
    up_weight,
    down_weight,
    prior_up_grad,
    prior_down_grad,
    master_up,
    master_down,
):
    columns = down_weight.shape[2]
    shape = (down_weight.shape[1] // (side * side * cores), columns)
    whole, line = (2, side, side, *shape), (2, side, *shape)
    turn, state, gots = 0, None, None

    def sum_turn():
        nonlocal turn, state, gots
        if turn == 0:
            up = prior_up_grad.reshape(side, side, cores, -1, prior_up_grad.shape[-1])
            down = prior_down_grad.reshape(side, side, cores, *shape)
            loads = pltpu.SemaphoreType.DMA((2 * (up.shape[-1] // columns + 1),))
            own, other = kernel(split_body, [(whole, bf16)] * 2, [(up, "far"), (down, "far")], [loads])
            state = own
            gots = lax.ppermute(other, "dp", by_position(2, lambda c: 1 - c))
        elif turn < 5:
            body = (halved_body, paired_body, crossing_body, paired_body)[turn - 1]
            out = ((2, *line), line, (2, 2, *shape), (2, *shape))[turn - 1]
            state, sent = kernel(body, [(out, bf16)] * 2, held(state, gots))
            gots = lax.ppermute(sent, "dp", by_position((turn - 1) // 2, near if turn % 2 else wrapped))
        else:
            masters = [(master_up[0], "copied"), (master_down[0], "copied")]
            outs = [(master_up.shape[1:], f32), (master_down.shape[1:], f32)]
            state = kernel(settled_body, outs, [*held(state, gots), *masters], plain=True)
        turn += 1

    sections = lax.axis_size("section")
    last, both, micros = sections - 1, range(lax.axis_size("tensor")), range(inputs.shape[0])
    count, width = inputs.shape[1:]
    w_up, w_down = up_weight[0], down_weight[0]
    hidden = w_up.shape[1]
    narrow, wide, broad = ((count, width), bf16), ((count, hidden), bf16), ((count, hidden), f32)
    packed = ((len(micros) * count, width), bf16)
    scratch = [pltpu.VMEM((count, hidden), bf16)]
    loads = pltpu.SemaphoreType.DMA((hidden // chunk + 3,))
    parts = [None for _ in micros]
    parts[0], inputs_here, gain_here, up_here, down_here = kernel(
        first_body,
        [narrow, (inputs.shape, bf16), (norm_gain.shape, f32), (w_up.shape, bf16), (w_down.shape, bf16)],
        [(inputs, "far"), (norm_gain, "far"), (w_up, "far"), (w_down, "far")],
        [*scratch, loads],
    )
    weights = held(gain_here, up_here, down_here)
    kept = [held(inputs_here)[0] for _ in micros]
    seeds = (out_grads, "copied")
    acts, slopes = [None for _ in micros], None
    rows, grads = [None for _ in micros], [None for _ in micros]
    stages = [*range(1, sections), *range(last - 1, -1, -1)]
    with_sum = (0, 1, 4, 5)
    backs = {}

    def opened(micro):
        (parts[micro],) = kernel(partial(opening_body, micro), [narrow], [*held(inputs_here), *weights], scratch)

    def stepped(at, micro, fresh):
        stage, down = stages[at], at >= last
        arrays = [*held(*fresh), kept[micro]]
        if at < last - 1:
            rows[micro], parts[micro] = kernel(
                partial(forward_body, stage, micro), [narrow, narrow], [*arrays, *weights], scratch
            )
            kept[micro] = (rows[micro], "held")
        elif not down:
            rows[micro], acts[micro], parts[micro] = kernel(
                partial(turn_body, stage, micro), [narrow, wide, narrow], [*arrays, seeds, *weights], scratch
            )
            kept[micro] = seeds
        else:
            grads[micro], parts[micro] = kernel(
                partial(backward_body, stage, micro),
                [narrow, narrow],
                [*arrays, *held(rows[micro], slopes[micro]), *weights],
                scratch,
            )
            kept[micro] = (grads[micro], "held")

    fresh = [None for _ in micros]
    for layer, stage in enumerate(stages):
        source = 0 if layer == 0 else stages[layer - 1]
        for micro in micros:
            if micro:
                opened(micro) if layer == 0 else stepped(layer - 1, micro, fresh[micro])
            fresh[micro] = hand_over(parts[micro], source, stage)
        if layer in with_sum:
            sum_turn()
        if layer == last:
            (mixed,) = kernel(
                partial(mix_body, last),
                [packed],
                held(*(array for both_of in zip(rows, acts) for array in both_of), down_here),
            )
            other = handed(mixed, [((last, t), (last, 1 - t)) for t in both])
            slopes = kernel(partial(slope_body, last), [broad for _ in micros], held(*rows, gain_here, up_here))
            (packed_rows,) = kernel(pack_body, [packed], held(*rows))
            backs[0] = handed(packed_rows, [((s + 1, t), (s, t)) for s in range(0, last, 2) for t in both])
        elif layer == last + 1:
            backs[1] = handed(packed_rows, [((s + 1, t), (s, t)) for s in range(1, last, 2) for t in both])
        elif layer == len(stages) - 1:
            (sent,) = kernel(pack_body, [packed], held(*grads))
            early = handed(sent, [((s, t), (s + 1, t)) for s in range(1, last, 2) for t in both])
        stepped(layer, 0, fresh[0])
    layer = len(stages)
    others = [None for _ in micros]
    for micro in micros:
        if micro:
            stepped(layer - 1, micro, fresh[micro])
        others[micro] = handed(parts[micro], [((0, t), (0, 1 - t)) for t in both])
    (sent,) = kernel(pack_body, [packed], held(*grads))
    late = handed(sent, [((s, t), (s + 1, t)) for s in range(0, last, 2) for t in both])
    sum_turn()
    sum_turn()
    returned = [backs[s % 2] for s in range(last)]
    (produced,) = kernel(produced_body, [packed], held(mixed, other, *returned), plain=True)
    ends = [array for both_halves in zip(parts, others) for array in both_halves]
    (grads_done,) = kernel(partial(grads_body, len(micros)), [packed], held(early, late, *ends), plain=True)
    new_up, new_down = state[0][None], state[1][None]
    whole_shape = (1, *inputs.shape)
    return (produced.reshape(whole_shape), grads_done.reshape(whole_shape), new_up, new_down)


def solution(mesh):
    placed = (
        P(None, "dp", None),
        P(None, "dp", None),
        P("section", None),
        P("section", None, "tensor"),
        P("section", "tensor", None),
        P("dp", "section", None, "tensor"),
        P("dp", "section", "tensor", None),
        P("section", "dp", "tensor"),
        P("section", ("tensor", "dp"), None),
    )
    return jax.shard_map(
        local,
        mesh=mesh,
        in_specs=placed,
        out_specs=(
            P("section", None, "dp", None),
            P("section", None, "dp", None),
            P("section", "dp", "tensor"),
            P("section", ("tensor", "dp"), None),
        ),
        check_vma=False,
    )
```

```python
from functools import partial

import jax
import jax.numpy as jnp
from jax import lax
from jax.experimental import pallas as pl
from jax.experimental.pallas import tpu as pltpu
from jax.sharding import PartitionSpec as P


eps_norm = 1e-05
gelu_coef = 0.7978845608028654
learning_rate = 0.05
bf16 = jnp.bfloat16
f32 = jnp.float32
side = 4
cores = 2


def hand_over(value, source, target):
    both = range(lax.axis_size("tensor"))
    crossed = handed(value, [((source, t), (target, 1 - t)) for t in both])
    straight = handed(value, [((source, t), (target, t)) for t in both])
    return straight, crossed


def handed(value, moves):
    halves = lax.axis_size("tensor")
    return lax.ppermute(
        value, ("section", "tensor"), [(a * halves + t, b * halves + u) for (a, t), (b, u) in moves]
    )


chunk = 512


def apply_norm(values):
    center = jnp.mean(values, axis=-1, keepdims=True)
    centered = values - center
    spread = jnp.mean(centered * centered, axis=-1, keepdims=True)
    inverse_scale = lax.rsqrt(spread + eps_norm)
    return centered * inverse_scale, inverse_scale


def plus(a, b):
    return (a.astype(f32) + b.astype(f32)).astype(bf16)


def chosen(stage, straight, crossed, kept):
    return jnp.where(lax.axis_index("section") == stage, plus(straight[...], crossed[...]), kept)


def up_of(normed, w_up, at):
    return jnp.dot(normed, w_up[:, at : at + chunk], preferred_element_type=f32)


def curve(upper):
    square = upper * upper
    return jnp.tanh(gelu_coef * (upper + 0.044715 * square * upper)), square


def rows_of(array, micro):
    return array[micro] if len(array.shape) == 3 else array[...]


def down_part(rows, act, w_down):
    part = jnp.dot(act[...], w_down[...], preferred_element_type=f32)
    return (part + 0.5 * rows.astype(f32)).astype(bf16)


def activate(rows, gain, w_up, act, ready=None):
    standardized, _ = apply_norm(rows.astype(f32))
    normed = (standardized * gain[...]).astype(bf16)
    for i, at in enumerate(range(0, act.shape[1], chunk)):
        if ready:
            ready[i].wait()
        upper = up_of(normed, w_up, at)
        inner, _ = curve(upper)
        act[:, at : at + chunk] = (0.5 * upper * (1.0 + inner)).astype(bf16)


def first_body(inputs, gain, w_up, w_down, part_out, inputs_here, gain_here, up_here, down_here, act, came):
    pairs = [(inputs, inputs_here), (gain, gain_here)]
    for at in range(0, act.shape[1], chunk):
        here = pl.ds(at, chunk)
        pairs.append((w_up.at[:, here], up_here.at[:, here]))
    pairs.append((w_down, down_here))
    loads = [pltpu.make_async_copy(a, b, came.at[i]) for i, (a, b) in enumerate(pairs)]
    first = lax.axis_index("section") == 0
    loads[0].start()
    loads[1].start()

    @pl.when(first)
    def _():
        for load in loads[2:]:
            load.start()

    loads[0].wait()
    loads[1].wait()

    @pl.when(first)
    def _():
        rows = inputs_here[0]
        activate(rows, gain_here, up_here, act, loads[2:-1])
        loads[-1].wait()
        part_out[...] = down_part(rows, act, down_here)


def fetch_body(after, w_up, w_down, up_in, down_in, up_here, down_here, came):
    loads = [
        pltpu.make_async_copy(w_up, up_here, came.at[0]),
        pltpu.make_async_copy(w_down, down_here, came.at[1]),
    ]

    @pl.when(lax.axis_index("section") > 0)
    def _():
        for load in loads:
            load.start()
        for load in loads:
            load.wait()


def at_section(stage):
    return pl.when(lax.axis_index("section") == stage)


def opening_body(micro, inputs, gain, w_up, w_down, part_out, act):
    @at_section(0)
    def _():
        rows = inputs[micro]
        activate(rows, gain, w_up, act)
        part_out[...] = down_part(rows, act, w_down)


def forward_body(stage, micro, straight, crossed, kept, gain, w_up, w_down, rows_out, part_out, act):
    rows = chosen(stage, straight, crossed, rows_of(kept, micro))
    rows_out[...] = rows

    @at_section(stage)
    def _():
        activate(rows, gain, w_up, act)
        part_out[...] = down_part(rows, act, w_down)


def grad_part(grad, pushed, standardized, inverse_scale, gain, w_up):
    part = lax.dot_general(pushed[...], w_up[...], across, preferred_element_type=f32) * gain
    leading = jnp.mean(part, axis=-1, keepdims=True)
    trailing = jnp.mean(part * standardized, axis=-1, keepdims=True)
    moved = inverse_scale * (part - leading - standardized * trailing)
    return (moved + 0.5 * grad.astype(f32)).astype(bf16)


across = (((1,), (1,)), ((), ()))


def slope_of(upper, inner, square):
    return 0.5 * (1.0 + inner) + 0.5 * upper * (1.0 - inner * inner) * gelu_coef * (1.0 + 3.0 * 0.044715 * square)


def turn_body(stage, micro, straight, crossed, kept, grad_in, gain, w_up, w_down, rows_out, act, part_out, pushed):
    rows = chosen(stage, straight, crossed, rows_of(kept, micro))
    rows_out[...] = rows

    @at_section(stage)
    def _():
        standardized, inverse_scale = apply_norm(rows.astype(f32))
        normed = (standardized * gain[...]).astype(bf16)
        grad = grad_in[micro]
        for at in range(0, act.shape[1], chunk):
            here = slice(at, at + chunk)
            upper = up_of(normed, w_up, at)
            inner, square = curve(upper)
            act[:, here] = (0.5 * upper * (1.0 + inner)).astype(bf16)
            grad_act = lax.dot_general(grad, w_down[here, :], across, preferred_element_type=f32)
            pushed[:, here] = (grad_act * slope_of(upper, inner, square)).astype(bf16)
        part_out[...] = grad_part(grad, pushed, standardized, inverse_scale, gain[...], w_up)


def slope_body(last, *refs):
    count = (len(refs) - 2) // 2
    gain, w_up = refs[count : count + 2]

    @pl.when(lax.axis_index("section") < last)
    def _():
        for rows, slope in zip(refs[:count], refs[count + 2 :]):
            standardized, _ = apply_norm(rows[...].astype(f32))
            normed = (standardized * gain[...]).astype(bf16)
            for at in range(0, slope.shape[1], chunk):
                upper = up_of(normed, w_up, at)
                inner, square = curve(upper)
                slope[:, at : at + chunk] = slope_of(upper, inner, square)


def backward_body(stage, micro, straight, crossed, kept, rows, slope, gain, w_up, w_down, grad_out, part_out, pushed):
    grad = chosen(stage, straight, crossed, rows_of(kept, micro))
    grad_out[...] = grad

    @at_section(stage)
    def _():
        for at in range(0, pushed.shape[1], chunk):
            here = slice(at, at + chunk)
            grad_act = lax.dot_general(grad, w_down[here, :], across, preferred_element_type=f32)
            pushed[:, here] = (grad_act * slope[:, here]).astype(bf16)
        standardized, inverse_scale = apply_norm(rows[...].astype(f32))
        part_out[...] = grad_part(grad, pushed, standardized, inverse_scale, gain[...], w_up)


def stacked(parts):
    return jnp.concatenate([part[...] for part in parts], axis=0)


def mix_body(last, token, *refs):
    *pairs, w_down, out = refs
    count = pairs[0].shape[0]

    @at_section(last)
    def _():
        for at in range(len(pairs) // 2):
            out[at * count : (at + 1) * count, :] = down_part(pairs[2 * at][...], pairs[2 * at + 1], w_down)


def pack_body(*refs):
    *parts, out = refs
    out[...] = stacked(parts)


def token_body(part, out):
    out[...] = part[: out.shape[0], : out.shape[1]]


def produced_body(last, mixed, other, back, out):
    out[...] = jnp.where(lax.axis_index("section") == last, plus(mixed[...], other[...]), back[...])


def grads_body(early, *refs):
    *ends, out = refs
    section = lax.axis_index("section")
    mine = jnp.concatenate([plus(a[...], b[...]) for a, b in zip(ends[::3], ends[1::3])], axis=0)
    back = jnp.where(lax.rem(section, 2) == 1, stacked(ends[2::3]), early[...])
    out[...] = jnp.where(section == 0, mine, back)


def held(*arrays):
    return [(array, "held") for array in arrays]


def kernel(body, outs, operands, scratch=(), plain=False, aliases={}):
    spaces = {"held": pltpu.VMEM, "copied": pltpu.VMEM, "far": pltpu.HBM}
    in_vmem = pl.BlockSpec(memory_space=pltpu.VMEM)
    return pl.pallas_call(
        body,
        out_shape=[(jax.ShapeDtypeStruct if plain else pltpu.VMEM)(shape, dtype) for shape, dtype in outs],
        in_specs=[pl.BlockSpec(memory_space=spaces[where]) for _, where in operands],
        out_specs=[in_vmem] * len(outs),
        scratch_shapes=list(scratch),
        input_output_aliases=aliases,
        compiler_params=pltpu.CompilerParams(vmem_limit_bytes=16 * 2**20),
    )(
        *(
            pltpu.with_memory_space_constraint(array, spaces[where]) if where in ("held", "far") else array
            for array, where in operands
        )
    )


def by_position(axis, move):
    pairs = []
    for x in range(side):
        for y in range(side):
            for core in range(cores):
                place = [x, y, core]
                place[axis] = move(place[axis])
                pairs.append(((x * side + y) * cores + core, (place[0] * side + place[1]) * cores + place[2]))
    return pairs


def near(position):
    return position ^ 1


def wrapped(position):
    return side - 1 - position


def my_core():
    return lax.rem(lax.axis_index("dp"), cores)


def my_places(axis):
    chip = lax.div(lax.axis_index("dp"), cores)
    own = lax.rem(chip, side) if axis else lax.div(chip, side)
    beside = near(own)
    return own, wrapped(own), beside, wrapped(beside)


def split_body(up, down, own, other, came):
    mine = my_core()
    rows, columns = up.shape[3], own.shape[-1]
    copies = []
    for to, core in ((own, mine), (other, cores - 1 - mine)):
        for part in range(up.shape[4] // columns):
            source = up.at[:, :, core, :, pl.ds(part * columns, columns)]
            copies.append((source, to.at[0, :, :, pl.ds(part * rows, rows), :]))
        copies.append((down.at[:, :, core], to.at[1]))
    copies = [pltpu.make_async_copy(a, b, came.at[i]) for i, (a, b) in enumerate(copies)]
    for copy in copies:
        copy.start()
    for copy in copies:
        copy.wait()


def halved_body(own, got, kept, sent):
    places = my_places(0)
    for slot in range(4):
        to = kept if slot < 2 else sent
        for weight in range(2):
            for line in range(side):
                block = (weight, places[slot], line)
                to[slot % 2, weight, line] = plus(own[block], got[block])


def paired_body(kept, got, mine, sent):
    mine[...] = plus(kept[0], got[0])
    sent[...] = plus(kept[1], got[1])


def crossing_body(mine, got, kept, sent):
    places = my_places(1)
    for slot in range(4):
        to = kept if slot < 2 else sent
        for weight in range(2):
            block = (weight, places[slot])
            to[slot % 2, weight] = plus(mine[block], got[block])


def settled_body(mine, got, master_up, master_down, new_up, new_down):
    rows, columns = master_up.shape[0], mine.shape[2]
    for part in range(master_up.shape[1] // columns):
        here, there = slice(part * rows, (part + 1) * rows), slice(part * columns, (part + 1) * columns)
        total = mine[0, here, :].astype(f32) + got[0, here, :].astype(f32)
        new_up[:, there] = master_up[:, there] - learning_rate * total
    total = mine[1].astype(f32) + got[1].astype(f32)
    new_down[...] = master_down[...] - learning_rate * total


def local(
    inputs,
    out_grads,
    norm_gain,
    up_weight,
    down_weight,
    prior_up_grad,
    prior_down_grad,
    master_up,
    master_down,
):
    columns = down_weight.shape[2]
    shape = (down_weight.shape[1] // (side * side * cores), columns)
    whole, line = (2, side, side, *shape), (2, side, *shape)
    turn, state, gots = 0, None, None

    def sum_turn():
        nonlocal turn, state, gots
        if turn == 0:
            up = prior_up_grad.reshape(side, side, cores, -1, prior_up_grad.shape[-1])
            down = prior_down_grad.reshape(side, side, cores, *shape)
            loads = pltpu.SemaphoreType.DMA((2 * (up.shape[-1] // columns + 1),))
            own, other = kernel(split_body, [(whole, bf16)] * 2, [(up, "far"), (down, "far")], [loads])
            state = own
            gots = lax.ppermute(other, "dp", by_position(2, lambda c: 1 - c))
        elif turn < 5:
            body = (halved_body, paired_body, crossing_body, paired_body)[turn - 1]
            out = ((2, *line), line, (2, 2, *shape), (2, *shape))[turn - 1]
            state, sent = kernel(body, [(out, bf16)] * 2, held(state, gots))
            gots = lax.ppermute(sent, "dp", by_position((turn - 1) // 2, near if turn % 2 else wrapped))
        else:
            masters = [(master_up[0], "copied"), (master_down[0], "copied")]
            outs = [(master_up.shape[1:], f32), (master_down.shape[1:], f32)]
            state = kernel(settled_body, outs, [*held(state, gots), *masters], plain=True)
        turn += 1

    sections = lax.axis_size("section")
    last, both, micros = sections - 1, range(lax.axis_size("tensor")), range(inputs.shape[0])
    count, width = inputs.shape[1:]
    w_up, w_down = up_weight[0], down_weight[0]
    hidden = w_up.shape[1]
    narrow, wide, broad = ((count, width), bf16), ((count, hidden), bf16), ((count, hidden), f32)
    packed = ((len(micros) * count, width), bf16)
    scratch = [pltpu.VMEM((count, hidden), bf16)]
    loads = pltpu.SemaphoreType.DMA((hidden // chunk + 3,))
    parts = [None for _ in micros]
    parts[0], inputs_here, gain_here, up_here, down_here = kernel(
        first_body,
        [narrow, (inputs.shape, bf16), (norm_gain.shape, f32), (w_up.shape, bf16), (w_down.shape, bf16)],
        [(inputs, "far"), (norm_gain, "far"), (w_up, "far"), (w_down, "far")],
        [*scratch, loads],
    )
    weights = held(gain_here, up_here, down_here)
    kept = [held(inputs_here)[0] for _ in micros]
    seeds = (out_grads, "copied")
    acts, slopes = [None for _ in micros], None
    rows, grads = [None for _ in micros], [None for _ in micros]
    stages = [*range(1, sections), *range(last - 1, -1, -1)]
    with_sum = (0, 1, 4, 5)

    def opened(micro):
        (parts[micro],) = kernel(partial(opening_body, micro), [narrow], [*held(inputs_here), *weights], scratch)

    def stepped(at, micro, fresh):
        stage, down = stages[at], at >= last
        arrays = [*held(*fresh), kept[micro]]
        if at < last - 1:
            rows[micro], parts[micro] = kernel(
                partial(forward_body, stage, micro), [narrow, narrow], [*arrays, *weights], scratch
            )
            kept[micro] = (rows[micro], "held")
        elif not down:
            rows[micro], acts[micro], parts[micro] = kernel(
                partial(turn_body, stage, micro), [narrow, wide, narrow], [*arrays, seeds, *weights], scratch
            )
            kept[micro] = seeds
        else:
            grads[micro], parts[micro] = kernel(
                partial(backward_body, stage, micro),
                [narrow, narrow],
                [*arrays, *held(rows[micro], slopes[micro]), *weights],
                scratch,
            )
            kept[micro] = (grads[micro], "held")

    fresh = [None for _ in micros]
    for layer, stage in enumerate(stages):
        source = 0 if layer == 0 else stages[layer - 1]
        for micro in micros:
            if micro:
                opened(micro) if layer == 0 else stepped(layer - 1, micro, fresh[micro])
            fresh[micro] = hand_over(parts[micro], source, stage)
        if layer in with_sum:
            sum_turn()
        if layer == 0:
            up_here, down_here = kernel(
                fetch_body,
                [(w_up.shape, bf16), (w_down.shape, bf16)],
                [*held(parts[-1]), (w_up, "far"), (w_down, "far"), *held(up_here, down_here)],
                [pltpu.SemaphoreType.DMA((2,))],
                aliases={3: 0, 4: 1},
            )
            weights = held(gain_here, up_here, down_here)
        if layer == last:
            slopes = kernel(partial(slope_body, last), [broad for _ in micros], held(*rows, gain_here, up_here))
            (packed_rows,) = kernel(pack_body, [packed], held(*rows))
        elif layer == last + 1:
            back = handed(packed_rows, [((s + 1, t), (s, t)) for s in range(last) for t in both])
        elif layer == len(stages) - 1:
            (token,) = kernel(token_body, [((16, 128), bf16)], held(parts[-1]))
            token = handed(token, [((1, t), (last, t)) for t in both])
            (sent,) = kernel(pack_body, [packed], held(*grads))
            early = handed(sent, [((s, t), (s + 1, t)) for s in range(1, last, 2) for t in both])
        stepped(layer, 0, fresh[0])
    layer = len(stages)
    others, lates = [None for _ in micros], [None for _ in micros]
    for micro in micros:
        if micro:
            stepped(layer - 1, micro, fresh[micro])
        others[micro] = handed(parts[micro], [((0, t), (0, 1 - t)) for t in both])
        lates[micro] = handed(grads[micro], [((s, t), (s + 1, t)) for s in range(0, last, 2) for t in both])
    (mixed,) = kernel(
        partial(mix_body, last),
        [packed],
        held(token, *(array for both_of in zip(rows, acts) for array in both_of), down_here),
    )
    other = handed(mixed, [((last, t), (last, 1 - t)) for t in both])
    sum_turn()
    sum_turn()
    (produced,) = kernel(partial(produced_body, last), [packed], held(mixed, other, back), plain=True)
    ends = [array for one_micro in zip(parts, others, lates) for array in one_micro]
    (grads_done,) = kernel(grads_body, [packed], held(early, *ends), plain=True)
    new_up, new_down = state[0][None], state[1][None]
    whole_shape = (1, *inputs.shape)
    return (produced.reshape(whole_shape), grads_done.reshape(whole_shape), new_up, new_down)


def solution(mesh):
    placed = (
        P(None, "dp", None),
        P(None, "dp", None),
        P("section", None),
        P("section", None, "tensor"),
        P("section", "tensor", None),
        P("dp", "section", None, "tensor"),
        P("dp", "section", "tensor", None),
        P("section", "dp", "tensor"),
        P("section", ("tensor", "dp"), None),
    )
    return jax.shard_map(
        local,
        mesh=mesh,
        in_specs=placed,
        out_specs=(
            P("section", None, "dp", None),
            P("section", None, "dp", None),
            P("section", "dp", "tensor"),
            P("section", ("tensor", "dp"), None),
        ),
        check_vma=False,
    )
```

```python
from functools import partial

import jax
import jax.numpy as jnp
from jax import lax
from jax.experimental import pallas as pl
from jax.experimental.pallas import tpu as pltpu
from jax.sharding import PartitionSpec as P


eps_norm = 1e-05
gelu_coef = 0.7978845608028654
learning_rate = 0.05
bf16 = jnp.bfloat16
f32 = jnp.float32
side = 4
cores = 2


def hand_over(value, source, target):
    both = range(lax.axis_size("tensor"))
    crossed = handed(value, [((source, t), (target, 1 - t)) for t in both])
    straight = handed(value, [((source, t), (target, t)) for t in both])
    return straight, crossed


def handed(value, moves):
    halves = lax.axis_size("tensor")
    return lax.ppermute(
        value, ("section", "tensor"), [(a * halves + t, b * halves + u) for (a, t), (b, u) in moves]
    )


chunk = 512
tile = 256


def apply_norm(values):
    center = jnp.mean(values, axis=-1, keepdims=True)
    centered = values - center
    spread = jnp.mean(centered * centered, axis=-1, keepdims=True)
    inverse_scale = lax.rsqrt(spread + eps_norm)
    return centered * inverse_scale, inverse_scale


def plus(a, b):
    return (a.astype(f32) + b.astype(f32)).astype(bf16)


def chosen(stage, straight, crossed, kept):
    return jnp.where(lax.axis_index("section") == stage, plus(straight[...], crossed[...]), kept)


def up_of(normed, w_up, at):
    return jnp.dot(normed, w_up[:, at : at + chunk], preferred_element_type=f32)


def curve(upper):
    square = upper * upper
    return jnp.tanh(gelu_coef * (upper + 0.044715 * square * upper)), square


def rows_of(array, micro):
    return array[micro] if len(array.shape) == 3 else array[...]


def down_part(rows, act, w_down):
    part = jnp.dot(act[...], w_down[...], preferred_element_type=f32)
    return (part + 0.5 * rows.astype(f32)).astype(bf16)


def activate(rows, gain, w_up, act, ready=None):
    standardized, _ = apply_norm(rows.astype(f32))
    normed = (standardized * gain[...]).astype(bf16)
    for i, at in enumerate(range(0, act.shape[1], chunk)):
        if ready:
            ready[i].wait()
        upper = up_of(normed, w_up, at)
        inner, _ = curve(upper)
        act[:, at : at + chunk] = (0.5 * upper * (1.0 + inner)).astype(bf16)


def first_body(inputs, gain, w_up, w_down, part_out, inputs_here, gain_here, up_here, down_here, act, came):
    pairs = [(inputs, inputs_here), (gain, gain_here)]
    for at in range(0, act.shape[1], chunk):
        here = pl.ds(at, chunk)
        pairs.append((w_up.at[:, here], up_here.at[:, here]))
    pairs.append((w_down, down_here))
    loads = [pltpu.make_async_copy(a, b, came.at[i]) for i, (a, b) in enumerate(pairs)]

    @pl.when(lax.axis_index("section") == 0)
    def _():
        for load in loads:
            load.start()
        loads[0].wait()
        loads[1].wait()
        rows = inputs_here[0]
        activate(rows, gain_here, up_here, act, loads[2:-1])
        loads[-1].wait()
        part_out[...] = down_part(rows, act, down_here)


def fetch_body(after, gain, w_up, w_down, gain_in, up_in, down_in, gain_here, up_here, down_here, came):
    pairs = ((gain, gain_here), (w_up, up_here), (w_down, down_here))
    loads = [pltpu.make_async_copy(a, b, came.at[i]) for i, (a, b) in enumerate(pairs)]

    @pl.when(lax.axis_index("section") > 0)
    def _():
        for load in loads:
            load.start()
        for load in loads:
            load.wait()


def flip_body(w_up, w_down, up_flip, down_flip):
    for weight, flip in ((w_up, up_flip), (w_down, down_flip)):
        for row in range(0, weight.shape[0], tile):
            for column in range(0, weight.shape[1], tile):
                flip[column : column + tile, row : row + tile] = weight[row : row + tile, column : column + tile].T


def at_section(stage):
    return pl.when(lax.axis_index("section") == stage)


def opening_body(micro, inputs, gain, w_up, w_down, part_out, act):
    @at_section(0)
    def _():
        rows = inputs[micro]
        activate(rows, gain, w_up, act)
        part_out[...] = down_part(rows, act, w_down)


def forward_body(stage, micro, straight, crossed, kept, gain, w_up, w_down, rows_out, part_out, act):
    rows = chosen(stage, straight, crossed, rows_of(kept, micro))
    rows_out[...] = rows

    @at_section(stage)
    def _():
        activate(rows, gain, w_up, act)
        part_out[...] = down_part(rows, act, w_down)


def grad_part(grad, pushed, standardized, inverse_scale, gain, up_flip):
    part = jnp.dot(pushed[...], up_flip[...], preferred_element_type=f32) * gain
    leading = jnp.mean(part, axis=-1, keepdims=True)
    trailing = jnp.mean(part * standardized, axis=-1, keepdims=True)
    moved = inverse_scale * (part - leading - standardized * trailing)
    return (moved + 0.5 * grad.astype(f32)).astype(bf16)


def slope_of(upper, inner, square):
    return 0.5 * (1.0 + inner) + 0.5 * upper * (1.0 - inner * inner) * gelu_coef * (1.0 + 3.0 * 0.044715 * square)


def turn_body(stage, micro, straight, crossed, kept, grad_in, gain, w_up, up_flip, down_flip, rows_out, act, part_out, pushed):
    rows = chosen(stage, straight, crossed, rows_of(kept, micro))
    rows_out[...] = rows

    @at_section(stage)
    def _():
        standardized, inverse_scale = apply_norm(rows.astype(f32))
        normed = (standardized * gain[...]).astype(bf16)
        grad = grad_in[micro]
        for at in range(0, act.shape[1], chunk):
            here = slice(at, at + chunk)
            upper = up_of(normed, w_up, at)
            inner, square = curve(upper)
            act[:, here] = (0.5 * upper * (1.0 + inner)).astype(bf16)
            grad_act = jnp.dot(grad, down_flip[:, here], preferred_element_type=f32)
            pushed[:, here] = (grad_act * slope_of(upper, inner, square)).astype(bf16)
        part_out[...] = grad_part(grad, pushed, standardized, inverse_scale, gain[...], up_flip)


def slope_body(last, *refs):
    count = (len(refs) - 2) // 2
    gain, w_up = refs[count : count + 2]

    @pl.when(lax.axis_index("section") < last)
    def _():
        for rows, slope in zip(refs[:count], refs[count + 2 :]):
            standardized, _ = apply_norm(rows[...].astype(f32))
            normed = (standardized * gain[...]).astype(bf16)
            for at in range(0, slope.shape[1], chunk):
                upper = up_of(normed, w_up, at)
                inner, square = curve(upper)
                slope[:, at : at + chunk] = slope_of(upper, inner, square)


def backward_body(stage, micro, straight, crossed, kept, rows, slope, gain, up_flip, down_flip, grad_out, part_out, pushed):
    grad = chosen(stage, straight, crossed, rows_of(kept, micro))
    grad_out[...] = grad

    @at_section(stage)
    def _():
        for at in range(0, pushed.shape[1], chunk):
            here = slice(at, at + chunk)
            grad_act = jnp.dot(grad, down_flip[:, here], preferred_element_type=f32)
            pushed[:, here] = (grad_act * slope[:, here]).astype(bf16)
        standardized, inverse_scale = apply_norm(rows[...].astype(f32))
        part_out[...] = grad_part(grad, pushed, standardized, inverse_scale, gain[...], up_flip)


def stacked(parts):
    return jnp.concatenate([part[...] for part in parts], axis=0)


def mix_body(last, token, *refs):
    *pairs, w_down, out = refs
    count = pairs[0].shape[0]

    @at_section(last)
    def _():
        for at in range(len(pairs) // 2):
            out[at * count : (at + 1) * count, :] = down_part(pairs[2 * at][...], pairs[2 * at + 1], w_down)


def pack_body(*refs):
    *parts, out = refs
    out[...] = stacked(parts)


def token_body(part, out):
    out[...] = part[: out.shape[0], : out.shape[1]]


def produced_body(last, mixed, other, back, out):
    out[...] = jnp.where(lax.axis_index("section") == last, plus(mixed[...], other[...]), back[...])


def grads_body(early, *refs):
    *ends, out = refs
    section = lax.axis_index("section")
    mine = jnp.concatenate([plus(a[...], b[...]) for a, b in zip(ends[::3], ends[1::3])], axis=0)
    back = jnp.where(lax.rem(section, 2) == 1, stacked(ends[2::3]), early[...])
    out[...] = jnp.where(section == 0, mine, back)


def held(*arrays):
    return [(array, "held") for array in arrays]


def kernel(body, outs, operands, scratch=(), plain=False, aliases={}):
    spaces = {"held": pltpu.VMEM, "copied": pltpu.VMEM, "far": pltpu.HBM}
    in_vmem = pl.BlockSpec(memory_space=pltpu.VMEM)
    return pl.pallas_call(
        body,
        out_shape=[(jax.ShapeDtypeStruct if plain else pltpu.VMEM)(shape, dtype) for shape, dtype in outs],
        in_specs=[pl.BlockSpec(memory_space=spaces[where]) for _, where in operands],
        out_specs=[in_vmem] * len(outs),
        scratch_shapes=list(scratch),
        input_output_aliases=aliases,
        compiler_params=pltpu.CompilerParams(vmem_limit_bytes=16 * 2**20),
    )(
        *(
            pltpu.with_memory_space_constraint(array, spaces[where]) if where in ("held", "far") else array
            for array, where in operands
        )
    )


def by_position(axis, move):
    pairs = []
    for x in range(side):
        for y in range(side):
            for core in range(cores):
                place = [x, y, core]
                place[axis] = move(place[axis])
                pairs.append(((x * side + y) * cores + core, (place[0] * side + place[1]) * cores + place[2]))
    return pairs


def near(position):
    return position ^ 1


def wrapped(position):
    return side - 1 - position


def my_core():
    return lax.rem(lax.axis_index("dp"), cores)


def my_places(axis):
    chip = lax.div(lax.axis_index("dp"), cores)
    own = lax.rem(chip, side) if axis else lax.div(chip, side)
    beside = near(own)
    return own, wrapped(own), beside, wrapped(beside)


def split_body(up, down, own, other, came):
    mine = my_core()
    rows, columns = up.shape[3], own.shape[-1]
    copies = []
    for to, core in ((own, mine), (other, cores - 1 - mine)):
        for part in range(up.shape[4] // columns):
            source = up.at[:, :, core, :, pl.ds(part * columns, columns)]
            copies.append((source, to.at[0, :, :, pl.ds(part * rows, rows), :]))
        copies.append((down.at[:, :, core], to.at[1]))
    copies = [pltpu.make_async_copy(a, b, came.at[i]) for i, (a, b) in enumerate(copies)]
    for copy in copies:
        copy.start()
    for copy in copies:
        copy.wait()


def halved_body(own, got, kept, sent):
    places = my_places(0)
    for slot in range(4):
        to = kept if slot < 2 else sent
        for weight in range(2):
            for line in range(side):
                block = (weight, places[slot], line)
                to[slot % 2, weight, line] = plus(own[block], got[block])


def paired_body(kept, got, mine, sent):
    mine[...] = plus(kept[0], got[0])
    sent[...] = plus(kept[1], got[1])


def crossing_body(mine, got, kept, sent):
    places = my_places(1)
    for slot in range(4):
        to = kept if slot < 2 else sent
        for weight in range(2):
            block = (weight, places[slot])
            to[slot % 2, weight] = plus(mine[block], got[block])


def settled_body(mine, got, master_up, master_down, new_up, new_down):
    rows, columns = master_up.shape[0], mine.shape[2]
    for part in range(master_up.shape[1] // columns):
        here, there = slice(part * rows, (part + 1) * rows), slice(part * columns, (part + 1) * columns)
        total = mine[0, here, :].astype(f32) + got[0, here, :].astype(f32)
        new_up[:, there] = master_up[:, there] - learning_rate * total
    total = mine[1].astype(f32) + got[1].astype(f32)
    new_down[...] = master_down[...] - learning_rate * total


def local(
    inputs,
    out_grads,
    norm_gain,
    up_weight,
    down_weight,
    prior_up_grad,
    prior_down_grad,
    master_up,
    master_down,
):
    columns = down_weight.shape[2]
    shape = (down_weight.shape[1] // (side * side * cores), columns)
    whole, line = (2, side, side, *shape), (2, side, *shape)
    turn, state, gots = 0, None, None

    def sum_turn():
        nonlocal turn, state, gots
        if turn == 0:
            up = prior_up_grad.reshape(side, side, cores, -1, prior_up_grad.shape[-1])
            down = prior_down_grad.reshape(side, side, cores, *shape)
            loads = pltpu.SemaphoreType.DMA((2 * (up.shape[-1] // columns + 1),))
            own, other = kernel(split_body, [(whole, bf16)] * 2, [(up, "far"), (down, "far")], [loads])
            state = own
            gots = lax.ppermute(other, "dp", by_position(2, lambda c: 1 - c))
        elif turn < 5:
            body = (halved_body, paired_body, crossing_body, paired_body)[turn - 1]
            out = ((2, *line), line, (2, 2, *shape), (2, *shape))[turn - 1]
            state, sent = kernel(body, [(out, bf16)] * 2, held(state, gots))
            gots = lax.ppermute(sent, "dp", by_position((turn - 1) // 2, near if turn % 2 else wrapped))
        else:
            masters = [(master_up[0], "copied"), (master_down[0], "copied")]
            outs = [(master_up.shape[1:], f32), (master_down.shape[1:], f32)]
            state = kernel(settled_body, outs, [*held(state, gots), *masters], plain=True)
        turn += 1

    sections = lax.axis_size("section")
    last, both, micros = sections - 1, range(lax.axis_size("tensor")), range(inputs.shape[0])
    count, width = inputs.shape[1:]
    w_up, w_down = up_weight[0], down_weight[0]
    hidden = w_up.shape[1]
    narrow, wide, broad = ((count, width), bf16), ((count, hidden), bf16), ((count, hidden), f32)
    packed = ((len(micros) * count, width), bf16)
    scratch = [pltpu.VMEM((count, hidden), bf16)]
    loads = pltpu.SemaphoreType.DMA((hidden // chunk + 3,))
    parts = [None for _ in micros]
    parts[0], inputs_here, gain_here, up_here, down_here = kernel(
        first_body,
        [narrow, (inputs.shape, bf16), (norm_gain.shape, f32), (w_up.shape, bf16), (w_down.shape, bf16)],
        [(inputs, "far"), (norm_gain, "far"), (w_up, "far"), (w_down, "far")],
        [*scratch, loads],
    )
    weights, flips = held(gain_here, up_here, down_here), None
    kept = [held(inputs_here)[0] for _ in micros]
    seeds = (out_grads, "copied")
    acts, slopes = [None for _ in micros], None
    rows, grads = [None for _ in micros], [None for _ in micros]
    stages = [*range(1, sections), *range(last - 1, -1, -1)]
    with_sum = (0, 1, 4, 5)

    def opened(micro):
        (parts[micro],) = kernel(partial(opening_body, micro), [narrow], [*held(inputs_here), *weights], scratch)

    def stepped(at, micro, fresh):
        stage, down = stages[at], at >= last
        arrays = [*held(*fresh), kept[micro]]
        if at < last - 1:
            rows[micro], parts[micro] = kernel(
                partial(forward_body, stage, micro), [narrow, narrow], [*arrays, *weights], scratch
            )
            kept[micro] = (rows[micro], "held")
        elif not down:
            rows[micro], acts[micro], parts[micro] = kernel(
                partial(turn_body, stage, micro),
                [narrow, wide, narrow],
                [*arrays, seeds, *weights[:2], *flips],
                scratch,
            )
            kept[micro] = seeds
        else:
            grads[micro], parts[micro] = kernel(
                partial(backward_body, stage, micro),
                [narrow, narrow],
                [*arrays, *held(rows[micro], slopes[micro]), weights[0], *flips],
                scratch,
            )
            kept[micro] = (grads[micro], "held")

    fresh = [None for _ in micros]
    for layer, stage in enumerate(stages):
        source = 0 if layer == 0 else stages[layer - 1]
        for micro in micros:
            if micro:
                opened(micro) if layer == 0 else stepped(layer - 1, micro, fresh[micro])
            fresh[micro] = hand_over(parts[micro], source, stage)
        if layer in with_sum:
            sum_turn()
        if layer == 0:
            gain_here, up_here, down_here = kernel(
                fetch_body,
                [(norm_gain.shape, f32), (w_up.shape, bf16), (w_down.shape, bf16)],
                [
                    *held(parts[-1]),
                    *((array, "far") for array in (norm_gain, w_up, w_down)),
                    *held(gain_here, up_here, down_here),
                ],
                [pltpu.SemaphoreType.DMA((3,))],
                aliases={4: 0, 5: 1, 6: 2},
            )
            weights = held(gain_here, up_here, down_here)
            flips = held(
                *kernel(flip_body, [(w_up.shape[::-1], bf16), (w_down.shape[::-1], bf16)], held(up_here, down_here))
            )
        if layer == last:
            slopes = kernel(partial(slope_body, last), [broad for _ in micros], held(*rows, gain_here, up_here))
            (packed_rows,) = kernel(pack_body, [packed], held(*rows))
        elif layer == len(stages) - 1:
            (token,) = kernel(token_body, [((16, 128), bf16)], held(parts[-1]))
            token = handed(token, [((1, t), (last, t)) for t in both])
            (sent,) = kernel(pack_body, [packed], held(*grads))
            back = handed(packed_rows, [((s + 1, t), (s, t)) for s in range(last) for t in both])
            early = handed(sent, [((s, t), (s + 1, t)) for s in range(1, last, 2) for t in both])
        stepped(layer, 0, fresh[0])
    layer = len(stages)
    others, lates = [None for _ in micros], [None for _ in micros]
    for micro in micros:
        if micro:
            stepped(layer - 1, micro, fresh[micro])
        others[micro] = handed(parts[micro], [((0, t), (0, 1 - t)) for t in both])
        lates[micro] = handed(grads[micro], [((s, t), (s + 1, t)) for s in range(0, last, 2) for t in both])
    (mixed,) = kernel(
        partial(mix_body, last),
        [packed],
        held(token, *(array for both_of in zip(rows, acts) for array in both_of), down_here),
    )
    other = handed(mixed, [((last, t), (last, 1 - t)) for t in both])
    sum_turn()
    sum_turn()
    (produced,) = kernel(partial(produced_body, last), [packed], held(mixed, other, back), plain=True)
    ends = [array for one_micro in zip(parts, others, lates) for array in one_micro]
    (grads_done,) = kernel(grads_body, [packed], held(early, *ends), plain=True)
    new_up, new_down = state[0][None], state[1][None]
    whole_shape = (1, *inputs.shape)
    return (produced.reshape(whole_shape), grads_done.reshape(whole_shape), new_up, new_down)


def solution(mesh):
    placed = (
        P(None, "dp", None),
        P(None, "dp", None),
        P("section", None),
        P("section", None, "tensor"),
        P("section", "tensor", None),
        P("dp", "section", None, "tensor"),
        P("dp", "section", "tensor", None),
        P("section", "dp", "tensor"),
        P("section", ("tensor", "dp"), None),
    )
    return jax.shard_map(
        local,
        mesh=mesh,
        in_specs=placed,
        out_specs=(
            P("section", None, "dp", None),
            P("section", None, "dp", None),
            P("section", "dp", "tensor"),
            P("section", ("tensor", "dp"), None),
        ),
        check_vma=False,
    )
```
